32 devices in a mesh: row: 4 (over y, core), col: 8 (over z, x).
Axes of the slice: x: 2, y: 2, z: 4, core: 2. Of those that a mesh axis runs over, the one named last changes fastest.
Arguments:
- right_sides: bfloat16 [1024, 32, 256], P('col', 'row'), may hold values from -6 to 6
- prior_left: bfloat16 [32, 32, 48, 1024], P('row', 'col'), may hold values from -0.21875 to 0.21875
- prior_right: bfloat16 [32, 32, 48, 1024], P('row', 'col'), may hold values from -0.1875 to 0.1875
- solved_prior: bfloat16 [32, 1024, 256], P('col', 'row'), may hold values from -6 to 6
- diag_left: bfloat16 [32, 4, 48, 1024], P('row', None, None, 'col'), may hold values from -0.4375 to 0.4375
- diag_right: bfloat16 [32, 4, 48, 1024], P('row', None, None, 'col'), may hold values from -0.1875 to 0.1875
- diag_inverse: bfloat16 [4, 1024, 1024], P(None, 'col'), may hold values from -1 to 2, as said below
Outputs:
- updated: float32 [1024, 32, 256], P('col', 'row')
- solved: bfloat16 [4, 1024, 256], P(None, 'col')
The draws below stay inside these ranges and needn't reach their ends.
Inputs may be any that keep to these rules, and one draw needn't show every extreme that they name: `diag_inverse`: each tile is lower triangular.
All inputs are finite; a program needn't handle non-finite values.
Results may differ from the reference program's by a relative error of at most 0.012.
Values may be sent and summed in bfloat16 or wider, within the bound.
No kernel may reach another device: no remote copies, remote signals or barrier semaphores. Data moves between devices by JAX's collectives and lax.ppermute only.
A program may use at most 64 MiB of HBM per device.

```python
import math
import jax
import jax.numpy as jnp
from jax import lax

TILE = 1024
RANK = 48
RHS = 256
STEPS = 4
RDEV = 8
ROWS = 32
PRIOR = 32
N_ROW = 4


def draw_diag_inverse(key, part):
    noise_key = jax.random.fold_in(key, 11)
    scale_key = jax.random.fold_in(key, 12)
    noise = jax.random.truncated_normal(noise_key, -4.0, 4.0, (STEPS, TILE, TILE), jnp.float32) * (0.5 / math.sqrt(TILE))
    lower = jnp.tril(noise, -1)
    scales = jax.random.uniform(scale_key, (STEPS, TILE), jnp.float32, 0.6, 1.6)
    eye_mat = jnp.eye(TILE, dtype=jnp.float32)
    return (lower + eye_mat[None, :, :] * scales[:, :, None]).astype(jnp.bfloat16)


def spiked(values, own_key, source, target, blocks, factor):
    def block_of(dim):
        return (jnp.arange(values.shape[dim]) // (values.shape[dim] // blocks)).reshape((-1,) + (1,) * (values.ndim - 1 - dim))

    one_side = jax.random.permutation(own_key, blocks)[block_of(target)]
    second = (block_of(target) + blocks // 2) % blocks
    return jnp.where((block_of(source) == one_side) | (block_of(source) == second), factor * values, values)


def steps_of(key, shape, cuts, smallest, high):
    loudness = 1.0
    for axis_at, parts in cuts:
        steps = jax.random.uniform(jax.random.fold_in(jax.random.fold_in(key, 6), axis_at), (parts,), jnp.float32, smallest / len(cuts), high / len(cuts))
        loudness = loudness * jnp.repeat(jnp.exp(steps), shape[axis_at] // parts).reshape((-1,) + (1,) * (len(shape) - 1 - axis_at))
    return loudness


def bell_draw(key, dims, spread, limit, pieces=(), kind=jnp.bfloat16):
    loudness = steps_of(key, dims, pieces, -0.22, 0.18) if pieces else 1.0
    entries = jax.random.normal(key, dims, jnp.float32) * spread * loudness
    return jnp.minimum(jnp.maximum(entries, -limit), limit).astype(kind)


def gaussian_with(stream_key, extent, width, reach, pieces, heavy, kind=jnp.bfloat16):
    drawn = width * jax.random.normal(stream_key, extent, jnp.float32)
    if pieces:
        drawn = drawn * steps_of(stream_key, extent, pieces, -0.22, 0.18)
    return jnp.clip(spiked(drawn, jax.random.fold_in(stream_key, 3), *heavy), -reach, reach).astype(kind)


def setup_inputs(seed: int = 0) -> dict:
    seeds = jax.random.split(jax.random.key(seed), 8)
    right_sides = bell_draw(seeds[0], (TILE, ROWS, RHS), 1.0, 6.0, ((0, 8), (1, 4)))
    prior_left = gaussian_with(seeds[1], (ROWS, PRIOR, RANK, TILE), (RANK * PRIOR) ** -0.5, 0.21875, ((0, 4), (1, 8)), (1, 3, 8, 2.0))
    prior_right = bell_draw(seeds[2], (ROWS, PRIOR, RANK, TILE), TILE ** -0.5, 0.1875, ((0, 4), (1, 8)))
    solved_prior = bell_draw(seeds[3], (PRIOR, TILE, RHS), 1.0, 6.0, ((0, 8), (1, 4)))
    diag_left = bell_draw(seeds[4], (ROWS, STEPS, RANK, TILE), (RANK * STEPS) ** -0.5, 0.4375, ((0, 4), (3, 8)))
    diag_right = bell_draw(seeds[5], (ROWS, STEPS, RANK, TILE), TILE ** -0.5, 0.1875, ((0, 4), (3, 8)))
    diag_inverse = draw_diag_inverse(jax.random.fold_in(seeds[7], 71), 0)
    return dict(right_sides=right_sides, prior_left=prior_left, prior_right=prior_right, solved_prior=solved_prior, diag_left=diag_left, diag_right=diag_right, diag_inverse=diag_inverse)


def tile_index(position):
    return (position % RDEV) * N_ROW + position // RDEV


def rounded(values):
    return lax.optimization_barrier(values.astype(jnp.bfloat16)).astype(jnp.float32)


def reference(right_sides, prior_left, prior_right, solved_prior, diag_left, diag_right, diag_inverse):
    known = solved_prior.astype(jnp.float32)

    def prior_row(factors):
        left_row, right_row = factors
        coeff = rounded(jnp.einsum("prt,pth->prh", right_row.astype(jnp.float32), known, precision=lax.Precision.HIGHEST))
        return jnp.einsum("prt,prh->th", left_row.astype(jnp.float32), coeff, precision=lax.Precision.HIGHEST)

    prior = lax.map(prior_row, (prior_left, prior_right))
    base = right_sides.astype(jnp.float32) - jnp.transpose(prior, (1, 0, 2))
    positions = jnp.arange(ROWS, dtype=jnp.int32)
    tiles = tile_index(positions)
    near_list = []
    solved_list = []
    for step in range(STEPS):
        spot = step * RDEV
        current = base[:, spot]
        for earlier in range(step):
            current = current - jnp.einsum("rt,rh->th", diag_left[spot, earlier].astype(jnp.float32), near_list[earlier][spot], precision=lax.Precision.HIGHEST)
        answer = jnp.dot(diag_inverse[step], current.astype(jnp.bfloat16), preferred_element_type=jnp.float32).astype(jnp.bfloat16)
        solved_list.append(answer)
        near_list.append(rounded(jnp.einsum("irt,th->irh", diag_right[:, step].astype(jnp.float32), answer.astype(jnp.float32), precision=lax.Precision.HIGHEST)))
    total = jnp.zeros(base.shape, jnp.float32)
    for step in range(STEPS):
        gate = (tiles > step).astype(jnp.float32)
        total = total + jnp.einsum("irt,irh->tih", diag_left[:, step].astype(jnp.float32), near_list[step] * gate[:, None, None], precision=lax.Precision.HIGHEST)
    return base - total, jnp.stack(solved_list, 0)
```

```python
import jax
import jax.numpy as jnp
from jax import lax
from jax.sharding import PartitionSpec as P

BF = jnp.bfloat16
F32 = jnp.float32


def swap(value, axis, size, mask):
    return lax.ppermute(value, axis, [(i, i ^ mask) for i in range(size)])


def low_of(size):
    return 2 if size <= 8 else 4


def gather(value, axis, size, low):
    own = [value] + [swap(value, axis, size, m) for m in range(low, size, low)]
    result = [None] * size
    for at, piece in enumerate(own):
        result[at * low] = piece
        for m in range(1, low):
            result[at * low + m] = swap(piece, axis, size, m)
    return result


def scatter_sum(blocks, axis, size, low):
    kept = [blocks[at].astype(F32) for at in range(0, size, low)]
    for m in range(1, low):
        sent = jnp.stack([blocks[at + m] for at in range(0, size, low)], 0)
        got = swap(sent, axis, size, m)
        kept = [k + got[n].astype(F32) for n, k in enumerate(kept)]
    total = kept[0]
    for n in range(1, size // low):
        total = total + swap(kept[n].astype(BF), axis, size, n * low).astype(F32)
    return total


def pick(value, index, dim=0):
    return lax.dynamic_index_in_dim(value, index, dim, keepdims=False)


def cut(value, index, width, dim):
    return lax.dynamic_slice_in_dim(value, index * width, width, dim)


def local(n_row, n_col, right_sides, prior_left, prior_right, solved_prior, diag_left, diag_right, diag_inverse):
    ts, slots, sides = right_sides.shape
    js = prior_left.shape[1]
    rank, tile = prior_left.shape[2:]
    steps = diag_left.shape[1]
    r = lax.axis_index("row")
    c = lax.axis_index("col")
    own = jnp.minimum(r, steps - 1)
    low_c, low_r = low_of(n_col), 2
    chunk = slots * rank // n_col

    known = jnp.concatenate(gather(solved_prior, "row", n_row, low_r), 1)
    tb = tile // n_row
    pr = jnp.concatenate([cut(prior_right, r ^ d, tb, 3) for d in range(n_row)], 3)

    turned = [pick(diag_right, jnp.minimum(r ^ d, steps - 1), 1) for d in range(n_row)]
    factors = [turned[0]] + [swap(turned[d], "row", n_row, d) for d in range(1, n_row)]
    factors = jnp.stack(factors, 0)
    flat = factors.reshape(n_row, n_col, chunk, ts)
    right = [pick(flat, c ^ e, 1).reshape(n_row * chunk, ts) for e in range(n_col)]
    right = [right[0]] + [swap(right[e], "col", n_col, e) for e in range(1, n_col)]
    right = jnp.concatenate(right, 1)
    heads = factors[:, 0].reshape(n_row * rank, ts)
    heads = jnp.concatenate(gather(heads, "col", n_col, low_c), 1)

    inverse = pick(diag_inverse, own)
    inverse = jnp.concatenate([cut(inverse, c ^ e, ts, 1) for e in range(n_col)], 1)

    lead_left = [cut(prior_left[0], c ^ e, ts, 2) for e in range(n_col)]

    coeff = jnp.einsum("jth,jrt->jrh", known, pr[0], preferred_element_type=F32).astype(BF)
    parts = [
        jnp.einsum("jrh,jrt->ht", coeff, lead_left[e], preferred_element_type=F32).astype(BF)
        for e in range(n_col)
    ]
    lead = right_sides[:, 0].astype(F32).T - scatter_sum(parts, "col", n_col, low_c)
    lefts = diag_left[0, : steps - 1].reshape((steps - 1) * rank, ts)
    wide = jnp.concatenate([lead.astype(BF), lefts], 0)
    wide = jnp.concatenate(gather(wide, "col", n_col, low_c), 1)
    answer = jnp.einsum("ws,ts->wt", wide, inverse, preferred_element_type=F32).astype(BF)
    answers = gather(answer, "row", n_row, low_r)
    full = jnp.concatenate(gather(answer, "col", n_col, low_c), 1)
    near = jnp.einsum("qt,wt->qw", right, full, preferred_element_type=F32).astype(BF)
    near = near.reshape(n_row, chunk, -1)
    head = jnp.einsum("qt,wt->qw", heads, full, preferred_element_type=F32).astype(BF)
    head = head.reshape(n_row, rank, -1)
    near = jnp.stack([near[0]] + [swap(near[d], "row", n_row, d) for d in range(1, n_row)], 0)
    head = gather(head, "row", n_row, low_r)
    head = jnp.stack(head, 0)
    near = [pick(near, r ^ m).astype(F32) for m in range(steps)]
    heads_of = {}
    for m in range(steps):
        mine = pick(head, r ^ m)
        for k in range(m + 1, steps):
            heads_of[k, m] = mine[k ^ m].astype(F32)

    def fixed(value, m, known_c):
        out = value[:, :sides]
        for l in range(m):
            at = sides + l * rank
            out = out - jnp.dot(value[:, at : at + rank].astype(BF), known_c[m, l], preferred_element_type=F32)
        return out.astype(BF)

    known_c = {}
    for m in range(steps):
        for k in range(m + 1, steps):
            known_c[k, m] = fixed(heads_of[k, m], m, known_c)
    slot_of = (c * chunk + jnp.arange(chunk)) // rank
    mine = jnp.stack(
        [
            jnp.where((slot_of * n_row + r > m)[:, None], fixed(near[m], m, known_c), 0).astype(BF)
            for m in range(steps)
        ],
        0,
    )
    pieces = jnp.stack(gather(mine, "col", n_col, low_c), 0)
    pieces = jnp.stack([pick(pieces, c ^ n) for n in range(n_col)], 0)
    every = jnp.moveaxis(pieces, 0, 1).reshape(steps, slots, rank, sides)

    answers = jnp.stack(answers, 0)
    solved = []
    for m in range(steps):
        a = pick(answers, r ^ m).astype(F32)
        out = a[:sides].T
        for l in range(m):
            at = sides + l * rank
            out = out - jnp.einsum("rt,rh->th", a[at : at + rank].astype(BF), known_c[m, l], preferred_element_type=F32)
        solved.append(out.astype(BF))
    solved = jnp.stack(solved, 0)

    rest = jnp.einsum("jth,sjrt->sjrh", known, pr[1:], preferred_element_type=F32).astype(BF)
    rest = jnp.einsum("sjrt,sjrh->tsh", prior_left[1:], rest, preferred_element_type=F32).astype(BF)
    rest = lax.psum_scatter(rest, "col", scatter_dimension=0, tiled=True).astype(F32)
    base = jnp.concatenate([lead.T[:, None], right_sides[:, 1:].astype(F32) - rest], 1)
    updated = base - jnp.einsum("smrt,msrh->tsh", diag_left, every, preferred_element_type=F32)
    return updated, solved


def solution(mesh):
    n_row, n_col = mesh.shape["row"], mesh.shape["col"]
    in_specs = (
        P("col", "row", None),
        P("row", "col", None, None),
        P("row", "col", None, None),
        P("col", "row", None),
        P("row", None, None, "col"),
        P("row", None, None, "col"),
        P(None, "col", None),
    )
    out_specs = (P("col", "row", None), P(None, "col", None))

    def body(*args):
        return local(n_row, n_col, *args)

    return jax.shard_map(body, mesh=mesh, in_specs=in_specs, out_specs=out_specs, check_vma=False)
```

```python
import jax
import jax.numpy as jnp
from jax import lax
from jax.experimental import pallas as pl
from jax.experimental.pallas import tpu as pltpu
from jax.sharding import PartitionSpec as P


BF = jnp.bfloat16
F32 = jnp.float32
SMEM = pl.BlockSpec(memory_space=pltpu.SMEM)
VMEM = pl.BlockSpec(memory_space=pltpu.VMEM)


def swap(value, axis, size, mask):
    return lax.ppermute(value, axis, [(i, i ^ mask) for i in range(size)])


def low_of(size):
    return 2 if size <= 8 else 4


def gather(value, axis, size, low):
    own = [value] + [swap(value, axis, size, m) for m in range(low, size, low)]
    result = [None] * size
    for at, piece in enumerate(own):
        result[at * low] = piece
        for m in range(1, low):
            result[at * low + m] = swap(piece, axis, size, m)
    return result


def pick(value, index, dim=0):
    return lax.dynamic_index_in_dim(value, index, dim, keepdims=False)


def tn(a, b):
    return lax.dot_general(a, b, (((0,), (0,)), ((), ())), preferred_element_type=F32)


def nt(a, b):
    return lax.dot_general(a, b, (((1,), (1,)), ((), ())), preferred_element_type=F32)


def nn(a, b):
    return lax.dot_general(a, b, (((1,), (0,)), ((), ())), preferred_element_type=F32)


def sds(shape, dtype=BF):
    return jax.ShapeDtypeStruct(shape, dtype)


def cost(flops, size):
    return pl.CostEstimate(flops=flops, bytes_accessed=size, transcendentals=0)


def pack_left(idx, left, low, nz, ts):
    _, js, rank, tile = left.shape

    def kernel(idx_ref, in_ref, *outs):
        c = idx_ref[1]
        for m in range(low):
            for k in range(nz):
                at = pl.multiple_of((c ^ (m + k * low)) * ts, ts)
                outs[m][:, k * ts : (k + 1) * ts] = in_ref[0, :, :, pl.ds(at, ts)].reshape(js * rank, ts)

    return pl.pallas_call(
        kernel,
        grid=(1,),
        in_specs=[SMEM, pl.BlockSpec((1, js, rank, tile), lambda n: (0, 0, 0, 0))],
        out_specs=[pl.BlockSpec((js * rank, nz * ts), lambda n: (0, 0))] * low,
        out_shape=[sds((js * rank, nz * ts))] * low,
        cost_estimate=cost(10**6, js * rank * tile * 4),
        name="pack_left",
    )(idx, left)


def pack_right(right, side):
    slots, steps, rank, ts = right.shape
    sides = side.shape[2]

    def kernel(in_ref, side_ref, out_ref, first_ref):
        out_ref[:, :, :rank] = in_ref[...]
        for s in range(slots):
            out_ref[s, :, rank:] = in_ref[0]
        first_ref[...] = side_ref[:, 0, :].astype(F32).T

    return pl.pallas_call(
        kernel,
        in_specs=[VMEM] * 2,
        out_specs=[VMEM] * 2,
        out_shape=[sds((slots, steps, 2 * rank, ts)), sds((sides, ts), F32)],
        cost_estimate=cost(10**6, right.size * 6),
        name="pack_right",
    )(right, side)


def coefficients(idx, known, right, groups):
    n_row = len(known)
    slots, js, rank, tile = right.shape
    tb, sides = known[0].shape[1:]

    def kernel(idx_ref, right_ref, *refs):
        r = idx_ref[0]
        held = refs[-1]
        for d in range(n_row):
            held[:, pl.ds(pl.multiple_of((r ^ d) * tb, tb), tb)] = refs[d][...]
        for j in range(js):
            total = nn(right_ref[:, j].reshape(slots * rank, tile), held[j])
            total = total.astype(BF).reshape(slots, rank, sides)
            at = 0
            for n, count in enumerate(groups):
                refs[n_row + n][:, j * rank : (j + 1) * rank] = total[at : at + count]
                at += count

    return pl.pallas_call(
        kernel,
        in_specs=[SMEM] + [VMEM] * (n_row + 1),
        out_specs=[VMEM] * len(groups),
        out_shape=[sds((g, js * rank, sides)) for g in groups],
        scratch_shapes=[pltpu.VMEM((js, tile, sides), BF)],
        cost_estimate=cost(2 * slots * js * rank * tile * sides, right.size * 2 + n_row * known[0].size * 2),
        name="coefficients",
    )(idx, right, *known)


def lead_parts(coeffs, lefts, nz, ts):
    low = len(coeffs)
    sides = coeffs[0].shape[2]

    def kernel(*refs):
        total = tn(refs[0][0], refs[low][...])
        for m in range(1, low):
            total = total + tn(refs[m][0], refs[low + m][...])
        for k in range(nz):
            refs[2 * low + k][...] = total[:, k * ts : (k + 1) * ts].astype(BF)

    return pl.pallas_call(
        kernel,
        in_specs=[VMEM] * (2 * low),
        out_specs=[VMEM] * nz,
        out_shape=[sds((sides, ts))] * nz,
        cost_estimate=cost(2 * low * lefts[0].size * sides, 10**6),
        name="lead_parts",
    )(*coeffs, *lefts)


def rest_parts(idx, coeff, left, first, blocks, ts):
    count, ranks, sides = coeff.shape
    _, js, rank, tile = left.shape
    many = len(blocks[0])

    def kernel(idx_ref, coeff_ref, left_ref, *refs):
        c = idx_ref[1]
        held = refs[-1]
        flat = [e for block in blocks for e in block]
        for n, e in enumerate(flat):
            at = pl.multiple_of((c ^ e) * ts, ts)
            held[:, n * ts : (n + 1) * ts] = left_ref[0, :, :, pl.ds(at, ts)].reshape(ranks, ts)
        total = tn(coeff_ref[0], held[...])
        for n in range(len(flat)):
            refs[n // many][n % many, 0] = total[:, n * ts : (n + 1) * ts].astype(BF)

    return pl.pallas_call(
        kernel,
        grid=(count,),
        in_specs=[
            SMEM,
            pl.BlockSpec((1, ranks, sides), lambda s: (s, 0, 0)),
            pl.BlockSpec((1, js, rank, tile), lambda s: (s + first, 0, 0, 0)),
        ],
        out_specs=[pl.BlockSpec((many, 1, sides, ts), lambda s: (0, s, 0, 0))] * len(blocks),
        out_shape=[sds((many, count, sides, ts))] * len(blocks),
        scratch_shapes=[pltpu.VMEM((ranks, tile), BF)],
        cost_estimate=cost(2 * count * ranks * sides * tile, count * (ranks * (sides + tile) + tile * sides) * 2),
        name="rest_parts",
    )(idx, coeff, left)


def widen(parts, side, left, extra):
    count = len(parts)
    sides, ts = parts[0].shape
    rank = left.shape[2]

    def kernel(*refs):
        total = refs[0][...].astype(F32)
        for n in range(1, count):
            total = total + refs[n][...].astype(F32)
        lead = refs[count][...] - total
        refs[count + 2][:sides] = lead.astype(BF)
        refs[count + 2][sides:] = refs[count + 1][0, :extra].reshape(extra * rank, ts)
        refs[count + 3][...] = lead

    return pl.pallas_call(
        kernel,
        in_specs=[VMEM] * (count + 2),
        out_specs=[VMEM] * 2,
        out_shape=[sds((sides + extra * rank, ts)), sds((sides, ts), F32)],
        cost_estimate=cost(10**6, 10**6),
        name="widen",
    )(*parts, side, left)


def solve(idx, pieces, inverse):
    n_col = len(pieces)
    width, ts = pieces[0].shape
    _, _, tile = inverse.shape

    def kernel(idx_ref, inverse_ref, *refs):
        c = idx_ref[1]
        held = refs[-1]
        for e in range(n_col):
            held[:, pl.ds(pl.multiple_of((c ^ e) * ts, ts), ts)] = refs[e][...]
        refs[n_col][...] = nt(held[...], inverse_ref[idx_ref[2]]).astype(BF)

    return pl.pallas_call(
        kernel,
        in_specs=[SMEM, VMEM] + [VMEM] * n_col,
        out_specs=VMEM,
        out_shape=sds((width, ts)),
        scratch_shapes=[pltpu.VMEM((width, tile), BF)],
        cost_estimate=cost(2 * width * ts * tile, 2 * inverse.size + 2 * width * tile),
        name="solve",
    )(idx, inverse, *pieces)


def nears(idx, pieces, right, q, rank):
    n_col = len(pieces)
    n_row, _, both_ranks, _ = right.shape
    width, ts = pieces[0].shape
    tile = n_col * ts
    rows = q + (n_row - 1) * rank

    def kernel(idx_ref, right_ref, *refs):
        r, c = idx_ref[0], idx_ref[1]
        out, held, factor, both = refs[n_col : n_col + n_row], refs[-3], refs[-2], refs[-1]
        for e in range(n_col):
            held[:, pl.ds(pl.multiple_of((c ^ e) * ts, ts), ts)] = refs[e][...]
            factor[:, :, e * ts : (e + 1) * ts] = right_ref[:, e]
        product = nt(factor[...].reshape(n_row * both_ranks, tile), held[...])
        both[...] = product.astype(BF).reshape(n_row, both_ranks, width)
        for d in range(n_row):
            out[d][:q] = both[r ^ d, :q]
            for k in range(1, n_row):
                out[d][q + (k - 1) * rank : q + k * rank] = both[k, q:]

    return pl.pallas_call(
        kernel,
        in_specs=[SMEM] + [VMEM] * (n_col + 1),
        out_specs=[VMEM] * n_row,
        out_shape=[sds((rows, width))] * n_row,
        scratch_shapes=[
            pltpu.VMEM((width, tile), BF),
            pltpu.VMEM((n_row, both_ranks, tile), BF),
            pltpu.VMEM((n_row, both_ranks, width), BF),
        ],
        cost_estimate=cost(2 * n_row * both_ranks * width * tile, 10**6),
        name="nears",
    )(idx, right, *pieces)


def settle(idx, messages, steps, sides, q, rank, per):
    n_row = len(messages)
    rows, width = messages[0].shape

    def kernel(idx_ref, *refs):
        r, c = idx_ref[0], idx_ref[1]
        held = refs[n_row + 2]
        for d in range(n_row):
            held[r ^ d] = refs[d][...]
        final = {}

        def fixed(value, m):
            out = value[:, :sides].astype(F32)
            for l in range(m):
                at = sides + l * rank
                out = out - nn(value[:, at : at + rank], final[m, l])
            return out.astype(BF)

        at_final = 0
        for m in range(steps):
            for k in range(m + 1, steps):
                at = q + (k - 1) * rank
                final[k, m] = fixed(held[m, at : at + rank], m)
                refs[n_row + 1][at_final] = final[k, m]
                at_final += 1
        slot = c // per
        for m in range(steps):
            mine = fixed(held[m, :q], m)
            refs[n_row][m] = jnp.where(slot * n_row + r > m, mine, jnp.zeros_like(mine))

    return pl.pallas_call(
        kernel,
        in_specs=[SMEM] + [VMEM] * n_row,
        out_specs=[VMEM] * 2,
        out_shape=[sds((steps, q, sides)), sds((steps * (steps - 1) // 2, rank, sides))],
        scratch_shapes=[pltpu.VMEM((n_row, rows, width), BF)],
        cost_estimate=cost(10**8, 10**6),
        name="settle",
    )(idx, *messages)


def answer_of(idx, answers, final, steps, sides, rank):
    n_row = len(answers)
    width, ts = answers[0].shape

    def kernel(idx_ref, final_ref, *refs):
        r = idx_ref[0]
        held = refs[n_row + 1]
        for d in range(n_row):
            held[r ^ d] = refs[d][...]
        where, n = {}, 0
        for m in range(steps):
            for k in range(m + 1, steps):
                where[k, m] = n
                n += 1
        for m in range(steps):
            out = held[m, :sides].astype(F32).T
            for l in range(m):
                at = sides + l * rank
                out = out - tn(held[m, at : at + rank], final_ref[where[m, l]])
            refs[n_row][m] = out.astype(BF)

    return pl.pallas_call(
        kernel,
        in_specs=[SMEM, VMEM] + [VMEM] * n_row,
        out_specs=VMEM,
        out_shape=sds((steps, ts, sides)),
        scratch_shapes=[pltpu.VMEM((n_row, width, ts), BF)],
        cost_estimate=cost(10**8, 10**6),
        name="answer_of",
    )(idx, final, *answers)


def scatter_sum(blocks, axis, size, low):
    kept = [blocks[at].astype(F32) for at in range(0, size, low)]
    for m in range(1, low):
        sent = jnp.stack([blocks[at + m] for at in range(0, size, low)], 0)
        got = swap(sent, axis, size, m)
        kept = [k + got[n].astype(F32) for n, k in enumerate(kept)]
    total = kept[0]
    for n in range(1, size // low):
        total = total + swap(kept[n].astype(BF), axis, size, n * low).astype(F32)
    return total


def cut(value, index, width, dim):
    return lax.dynamic_slice_in_dim(value, index * width, width, dim)


def plain(n_row, n_col, right_sides, prior_left, prior_right, solved_prior, diag_left, diag_right, diag_inverse):
    ts, slots, sides = right_sides.shape
    rank, tile = prior_left.shape[2:]
    steps = diag_left.shape[1]
    r = lax.axis_index("row")
    c = lax.axis_index("col")
    own = jnp.minimum(r, steps - 1)
    low_c, low_r = low_of(n_col), 2
    chunk = slots * rank // n_col

    known = jnp.concatenate(gather(solved_prior, "row", n_row, low_r), 1)
    tb = tile // n_row
    pr = jnp.concatenate([cut(prior_right, r ^ d, tb, 3) for d in range(n_row)], 3)

    turned = [pick(diag_right, jnp.minimum(r ^ d, steps - 1), 1) for d in range(n_row)]
    factors = [turned[0]] + [swap(turned[d], "row", n_row, d) for d in range(1, n_row)]
    factors = jnp.stack(factors, 0)
    flat = factors.reshape(n_row, n_col, chunk, ts)
    right = [pick(flat, c ^ e, 1).reshape(n_row * chunk, ts) for e in range(n_col)]
    right = [right[0]] + [swap(right[e], "col", n_col, e) for e in range(1, n_col)]
    right = jnp.concatenate(right, 1)
    heads = factors[:, 0].reshape(n_row * rank, ts)
    heads = jnp.concatenate(gather(heads, "col", n_col, low_c), 1)

    inverse = pick(diag_inverse, own)
    inverse = jnp.concatenate([cut(inverse, c ^ e, ts, 1) for e in range(n_col)], 1)

    lead_left = [cut(prior_left[0], c ^ e, ts, 2) for e in range(n_col)]

    coeff = jnp.einsum("jth,jrt->jrh", known, pr[0], preferred_element_type=F32).astype(BF)
    parts = [
        jnp.einsum("jrh,jrt->ht", coeff, lead_left[e], preferred_element_type=F32).astype(BF)
        for e in range(n_col)
    ]
    lead = right_sides[:, 0].astype(F32).T - scatter_sum(parts, "col", n_col, low_c)
    lefts = diag_left[0, : steps - 1].reshape((steps - 1) * rank, ts)
    wide = jnp.concatenate([lead.astype(BF), lefts], 0)
    wide = jnp.concatenate(gather(wide, "col", n_col, low_c), 1)
    answer = jnp.einsum("ws,ts->wt", wide, inverse, preferred_element_type=F32).astype(BF)
    answers = gather(answer, "row", n_row, low_r)
    full = jnp.concatenate(gather(answer, "col", n_col, low_c), 1)
    near = jnp.einsum("qt,wt->qw", right, full, preferred_element_type=F32).astype(BF)
    near = near.reshape(n_row, chunk, -1)
    head = jnp.einsum("qt,wt->qw", heads, full, preferred_element_type=F32).astype(BF)
    head = head.reshape(n_row, rank, -1)
    near = jnp.stack([near[0]] + [swap(near[d], "row", n_row, d) for d in range(1, n_row)], 0)
    head = gather(head, "row", n_row, low_r)
    head = jnp.stack(head, 0)
    near = [pick(near, r ^ m).astype(F32) for m in range(steps)]
    heads_of = {}
    for m in range(steps):
        mine = pick(head, r ^ m)
        for k in range(m + 1, steps):
            heads_of[k, m] = mine[k ^ m].astype(F32)

    def fixed(value, m, known_c):
        out = value[:, :sides]
        for l in range(m):
            at = sides + l * rank
            out = out - jnp.dot(value[:, at : at + rank].astype(BF), known_c[m, l], preferred_element_type=F32)
        return out.astype(BF)

    known_c = {}
    for m in range(steps):
        for k in range(m + 1, steps):
            known_c[k, m] = fixed(heads_of[k, m], m, known_c)
    slot_of = (c * chunk + jnp.arange(chunk)) // rank
    mine = jnp.stack(
        [
            jnp.where((slot_of * n_row + r > m)[:, None], fixed(near[m], m, known_c), 0).astype(BF)
            for m in range(steps)
        ],
        0,
    )
    pieces = jnp.stack(gather(mine, "col", n_col, low_c), 0)
    pieces = jnp.stack([pick(pieces, c ^ n) for n in range(n_col)], 0)
    every = jnp.moveaxis(pieces, 0, 1).reshape(steps, slots, rank, sides)

    answers = jnp.stack(answers, 0)
    solved = []
    for m in range(steps):
        a = pick(answers, r ^ m).astype(F32)
        out = a[:sides].T
        for l in range(m):
            at = sides + l * rank
            out = out - jnp.einsum("rt,rh->th", a[at : at + rank].astype(BF), known_c[m, l], preferred_element_type=F32)
        solved.append(out.astype(BF))
    solved = jnp.stack(solved, 0)

    rest = jnp.einsum("jth,sjrt->sjrh", known, pr[1:], preferred_element_type=F32).astype(BF)
    rest = jnp.einsum("sjrt,sjrh->tsh", prior_left[1:], rest, preferred_element_type=F32).astype(BF)
    rest = lax.psum_scatter(rest, "col", scatter_dimension=0, tiled=True).astype(F32)
    base = jnp.concatenate([lead.T[:, None], right_sides[:, 1:].astype(F32) - rest], 1)
    updated = base - jnp.einsum("smrt,msrh->tsh", diag_left, every, preferred_element_type=F32)
    return updated, solved


def local(n_row, n_col, *args):
    right_sides, _, _, _, diag_left, _, _ = args
    ts, slots, _ = right_sides.shape
    steps = diag_left.shape[1]
    if ts % 128 or n_row != steps or n_col != slots:
        return plain(n_row, n_col, *args)
    return tiled(n_row, n_col, *args)


def tiled(n_row, n_col, right_sides, prior_left, prior_right, solved_prior, diag_left, diag_right, diag_inverse):
    ts, slots, sides = right_sides.shape
    rank = prior_left.shape[2]
    steps = diag_left.shape[1]
    r = lax.axis_index("row")
    c = lax.axis_index("col")
    idx = jnp.stack([r, c, r]).astype(jnp.int32)
    low = low_of(n_col)
    nz = n_col // low
    half = slots // 2
    groups = (1, half, slots - 1 - half)

    def send(value, axis, mask):
        return swap(value, axis, n_row if axis == "row" else n_col, mask)

    def spread(value, axis):
        size = n_row if axis == "row" else n_col
        result = [value] + [None] * (size - 1)
        mask = size // 2
        while mask:
            for at in range(0, size, 2 * mask):
                result[at + mask] = send(result[at], axis, mask)
            mask //= 2
        return result

    known = spread(solved_prior, "row")
    factors, side = pack_right(diag_right, right_sides)
    factors = lax.all_to_all(factors, "col", 0, 0)
    packed = pack_left(idx, prior_left, low, nz, ts)
    packed = [packed[0]] + [send(packed[m], "col", m) for m in range(1, low)]
    coeffs = coefficients(idx, known, prior_right, groups)
    leads = [coeffs[0]] + [send(coeffs[0], "col", m) for m in range(1, low)]
    factors = lax.all_to_all(jnp.transpose(factors, (1, 0, 2, 3)), "row", 0, 0)

    parts = lead_parts(leads, packed, nz, ts)
    parts = [parts[0]] + [send(parts[k], "col", k * low) for k in range(1, nz)]
    wide, lead = widen(parts, side, diag_left, steps - 1)
    wide = spread(wide, "col")
    answer = solve(idx, wide, diag_inverse)
    full = spread(answer, "col")
    answers = spread(answer, "row")
    messages = nears(idx, full, factors, rank, rank)
    messages = [messages[0]] + [send(messages[d], "row", d) for d in range(1, n_row)]
    mine, final = settle(idx, messages, steps, sides, rank, rank, 1)
    pieces = jnp.stack(spread(mine, "col"), 0)
    every = jnp.stack([pick(pieces, c ^ n) for n in range(n_col)], 0)
    solved = answer_of(idx, answers, final, steps, sides, rank)

    order = [0]
    while len(order) < nz:
        order = [2 * k for k in order] + [2 * k + 1 for k in order]
    blocks = [[m + k * low for k in order] for m in range(low)]
    rest = []
    for n in range(1, len(groups)):
        parts = rest_parts(idx, coeffs[n], prior_left, sum(groups[:n]), blocks, ts)
        gots = [send(parts[m], "col", m) for m in range(1, low)]
        kept, mask = parts[0], low
        while True:
            half = kept.shape[0] // 2
            if half == 0:
                break

            def added(part):
                total = kept[part].astype(F32)
                for got in gots:
                    total = total + got[part].astype(F32)
                return total.astype(BF)

            sent = added(slice(half, None))
            kept = added(slice(0, half))
            gots, mask = [send(sent, "col", mask)], 2 * mask
        rest.append(kept[0].astype(F32) + gots[0][0].astype(F32))
    rest = jnp.concatenate(rest, 0)
    base = jnp.concatenate([lead.T[:, None], right_sides[:, 1:].astype(F32) - jnp.transpose(rest, (2, 0, 1))], 1)
    updated = base - jnp.einsum("smrt,smrh->tsh", diag_left, every, preferred_element_type=F32)
    return updated, solved


def solution(mesh):
    n_row, n_col = mesh.shape["row"], mesh.shape["col"]
    in_specs = (
        P("col", "row", None),
        P("row", "col", None, None),
        P("row", "col", None, None),
        P("col", "row", None),
        P("row", None, None, "col"),
        P("row", None, None, "col"),
        P(None, "col", None),
    )
    out_specs = (P("col", "row", None), P(None, "col", None))

    def body(*args):
        return local(n_row, n_col, *args)

    return jax.shard_map(body, mesh=mesh, in_specs=in_specs, out_specs=out_specs, check_vma=False)
```

```python
import jax
import jax.numpy as jnp
from jax import lax
from jax.experimental import pallas as pl
from jax.experimental.pallas import tpu as pltpu
from jax.sharding import PartitionSpec as P


BF = jnp.bfloat16
F32 = jnp.float32
SMEM = pl.BlockSpec(memory_space=pltpu.SMEM)
VMEM = pl.BlockSpec(memory_space=pltpu.VMEM)


def swap(value, axis, size, mask):
    return lax.ppermute(value, axis, [(i, i ^ mask) for i in range(size)])


def low_of(size):
    return 2 if size <= 8 else 4


def gather(value, axis, size, low):
    own = [value] + [swap(value, axis, size, m) for m in range(low, size, low)]
    result = [None] * size
    for at, piece in enumerate(own):
        result[at * low] = piece
        for m in range(1, low):
            result[at * low + m] = swap(piece, axis, size, m)
    return result


def pick(value, index, dim=0):
    return lax.dynamic_index_in_dim(value, index, dim, keepdims=False)


def tn(a, b):
    return lax.dot_general(a, b, (((0,), (0,)), ((), ())), preferred_element_type=F32)


def nt(a, b):
    return lax.dot_general(a, b, (((1,), (1,)), ((), ())), preferred_element_type=F32)


def nn(a, b):
    return lax.dot_general(a, b, (((1,), (0,)), ((), ())), preferred_element_type=F32)


def sds(shape, dtype=BF):
    return jax.ShapeDtypeStruct(shape, dtype)


def cost(flops, size):
    return pl.CostEstimate(flops=flops, bytes_accessed=size, transcendentals=0)


def pack_left(idx, left, low, nz, ts):
    _, js, rank, tile = left.shape

    def kernel(idx_ref, in_ref, *outs):
        c = idx_ref[1]
        for m in range(low):
            for k in range(nz):
                at = pl.multiple_of((c ^ (m + k * low)) * ts, ts)
                outs[m][:, k * ts : (k + 1) * ts] = in_ref[0, :, :, pl.ds(at, ts)].reshape(js * rank, ts)

    return pl.pallas_call(
        kernel,
        grid=(1,),
        in_specs=[SMEM, pl.BlockSpec((1, js, rank, tile), lambda n: (0, 0, 0, 0))],
        out_specs=[pl.BlockSpec((js * rank, nz * ts), lambda n: (0, 0))] * low,
        out_shape=[sds((js * rank, nz * ts))] * low,
        cost_estimate=cost(10**6, js * rank * tile * 4),
        name="pack_left",
    )(idx, left)


def pack_right(right, side):
    slots, steps, rank, ts = right.shape
    sides = side.shape[2]

    def kernel(in_ref, side_ref, out_ref, first_ref):
        out_ref[:, :, :rank] = in_ref[...]
        for s in range(slots):
            out_ref[s, :, rank:] = in_ref[0]
        first_ref[...] = side_ref[:, 0, :].astype(F32).T

    return pl.pallas_call(
        kernel,
        in_specs=[VMEM] * 2,
        out_specs=[VMEM] * 2,
        out_shape=[sds((slots, steps, 2 * rank, ts)), sds((sides, ts), F32)],
        cost_estimate=cost(10**6, right.size * 6),
        name="pack_right",
    )(right, side)


def coefficients(idx, known, right, groups):
    n_row = len(known)
    slots, js, rank, tile = right.shape
    tb, sides = known[0].shape[1:]

    def kernel(idx_ref, right_ref, *refs):
        r = idx_ref[0]
        held = refs[-1]
        for d in range(n_row):
            held[:, pl.ds(pl.multiple_of((r ^ d) * tb, tb), tb)] = refs[d][...]
        for j in range(js):
            total = nn(right_ref[:, j].reshape(slots * rank, tile), held[j])
            total = total.astype(BF).reshape(slots, rank, sides)
            at = 0
            for n, count in enumerate(groups):
                refs[n_row + n][:, j * rank : (j + 1) * rank] = total[at : at + count]
                at += count

    return pl.pallas_call(
        kernel,
        in_specs=[SMEM] + [VMEM] * (n_row + 1),
        out_specs=[VMEM] * len(groups),
        out_shape=[sds((g, js * rank, sides)) for g in groups],
        scratch_shapes=[pltpu.VMEM((js, tile, sides), BF)],
        cost_estimate=cost(2 * slots * js * rank * tile * sides, right.size * 2 + n_row * known[0].size * 2),
        name="coefficients",
    )(idx, right, *known)


def lead_parts(coeffs, lefts, nz, ts):
    low = len(coeffs)
    sides = coeffs[0].shape[2]

    def kernel(*refs):
        total = tn(refs[0][0], refs[low][...])
        for m in range(1, low):
            total = total + tn(refs[m][0], refs[low + m][...])
        for k in range(nz):
            refs[2 * low + k][...] = total[:, k * ts : (k + 1) * ts].astype(BF)

    return pl.pallas_call(
        kernel,
        in_specs=[VMEM] * (2 * low),
        out_specs=[VMEM] * nz,
        out_shape=[sds((sides, ts))] * nz,
        cost_estimate=cost(2 * low * lefts[0].size * sides, 10**6),
        name="lead_parts",
    )(*coeffs, *lefts)


def rest_parts(idx, coeff, left, first, blocks, ts):
    count, ranks, sides = coeff.shape
    _, js, rank, tile = left.shape
    many = len(blocks[0])

    def kernel(idx_ref, coeff_ref, left_ref, *refs):
        c = idx_ref[1]
        held = refs[-1]
        flat = [e for block in blocks for e in block]
        for n, e in enumerate(flat):
            at = pl.multiple_of((c ^ e) * ts, ts)
            held[:, n * ts : (n + 1) * ts] = left_ref[0, :, :, pl.ds(at, ts)].reshape(ranks, ts)
        total = tn(coeff_ref[0], held[...])
        for n in range(len(flat)):
            refs[n // many][n % many, 0] = total[:, n * ts : (n + 1) * ts].astype(BF)

    return pl.pallas_call(
        kernel,
        grid=(count,),
        in_specs=[
            SMEM,
            pl.BlockSpec((1, ranks, sides), lambda s: (s, 0, 0)),
            pl.BlockSpec((1, js, rank, tile), lambda s: (s + first, 0, 0, 0)),
        ],
        out_specs=[pl.BlockSpec((many, 1, sides, ts), lambda s: (0, s, 0, 0))] * len(blocks),
        out_shape=[sds((many, count, sides, ts))] * len(blocks),
        scratch_shapes=[pltpu.VMEM((ranks, tile), BF)],
        cost_estimate=cost(2 * count * ranks * sides * tile, count * (ranks * (sides + tile) + tile * sides) * 2),
        name="rest_parts",
    )(idx, coeff, left)


def widen(parts, side, left, extra):
    count = len(parts)
    sides, ts = parts[0].shape
    rank = left.shape[2]

    def kernel(*refs):
        total = refs[0][...].astype(F32)
        for n in range(1, count):
            total = total + refs[n][...].astype(F32)
        lead = refs[count][...] - total
        refs[count + 2][:sides] = lead.astype(BF)
        refs[count + 2][sides:] = refs[count + 1][0, :extra].reshape(extra * rank, ts)
        refs[count + 3][...] = lead

    return pl.pallas_call(
        kernel,
        in_specs=[VMEM] * (count + 2),
        out_specs=[VMEM] * 2,
        out_shape=[sds((sides + extra * rank, ts)), sds((sides, ts), F32)],
        cost_estimate=cost(10**6, 10**6),
        name="widen",
    )(*parts, side, left)


def solve(idx, pieces, inverse):
    n_col = len(pieces)
    width, ts = pieces[0].shape
    _, _, tile = inverse.shape

    def kernel(idx_ref, inverse_ref, *refs):
        c = idx_ref[1]
        held = refs[-1]
        for e in range(n_col):
            held[:, pl.ds(pl.multiple_of((c ^ e) * ts, ts), ts)] = refs[e][...]
        refs[n_col][...] = nt(held[...], inverse_ref[idx_ref[2]]).astype(BF)

    return pl.pallas_call(
        kernel,
        in_specs=[SMEM, VMEM] + [VMEM] * n_col,
        out_specs=VMEM,
        out_shape=sds((width, ts)),
        scratch_shapes=[pltpu.VMEM((width, tile), BF)],
        cost_estimate=cost(2 * width * ts * tile, 2 * inverse.size + 2 * width * tile),
        name="solve",
    )(idx, inverse, *pieces)


def folded(width, rank, q):
    keep = width // 128 * 128
    return keep if q <= rank and width - rank + (width - keep) <= keep else width


def nears(idx, pieces, right, q, rank):
    n_col = len(pieces)
    n_row, _, both_ranks, _ = right.shape
    width, ts = pieces[0].shape
    tile = n_col * ts
    rows = q + (n_row - 1) * rank
    keep = folded(width, rank, q)

    def kernel(idx_ref, right_ref, *refs):
        r, c = idx_ref[0], idx_ref[1]
        out, held, factor, both = refs[n_col : n_col + n_row], refs[-3], refs[-2], refs[-1]
        for e in range(n_col):
            held[:, pl.ds(pl.multiple_of((c ^ e) * ts, ts), ts)] = refs[e][...]
            factor[:, :, e * ts : (e + 1) * ts] = right_ref[:, e]
        product = nt(factor[...].reshape(n_row * both_ranks, tile), held[...])
        both[...] = product.astype(BF).reshape(n_row, both_ranks, width)
        for d in range(n_row):
            out[d][:q] = both[r ^ d, :q, :keep]
            for k in range(1, n_row):
                out[d][q + (k - 1) * rank : q + k * rank] = both[k, q:, :keep]
            if keep < width:
                out[d][q : 2 * q, width - rank : width - rank + width - keep] = both[r ^ d, :q, keep:]

    return pl.pallas_call(
        kernel,
        in_specs=[SMEM] + [VMEM] * (n_col + 1),
        out_specs=[VMEM] * n_row,
        out_shape=[sds((rows, keep))] * n_row,
        scratch_shapes=[
            pltpu.VMEM((width, tile), BF),
            pltpu.VMEM((n_row, both_ranks, tile), BF),
            pltpu.VMEM((n_row, both_ranks, width), BF),
        ],
        cost_estimate=cost(2 * n_row * both_ranks * width * tile, 10**6),
        name="nears",
    )(idx, right, *pieces)


def settle(idx, messages, steps, sides, q, rank, per):
    n_row = len(messages)
    rows, keep = messages[0].shape
    width = sides + (steps - 1) * rank

    def kernel(idx_ref, *refs):
        r, c = idx_ref[0], idx_ref[1]
        held = refs[n_row + 2]
        for d in range(n_row):
            held[r ^ d] = refs[d][...]
        final = {}

        def fixed(value, m):
            out = value[:, :sides].astype(F32)
            for l in range(m):
                at = sides + l * rank
                out = out - nn(value[:, at : at + rank], final[m, l])
            return out.astype(BF)

        at_final = 0
        for m in range(steps):
            for k in range(m + 1, steps):
                at = q + (k - 1) * rank
                final[k, m] = fixed(held[m, at : at + rank], m)
                refs[n_row + 1][at_final] = final[k, m]
                at_final += 1
        slot = c // per
        for m in range(steps):
            mine = held[m, :q]
            if keep < width and m == steps - 1:
                mine = jnp.concatenate([mine, held[m, q : 2 * q, width - rank : width - rank + width - keep]], 1)
            mine = fixed(mine, m)
            refs[n_row][m] = jnp.where(slot * n_row + r > m, mine, jnp.zeros_like(mine))

    return pl.pallas_call(
        kernel,
        in_specs=[SMEM] + [VMEM] * n_row,
        out_specs=[VMEM] * 2,
        out_shape=[sds((steps, q, sides)), sds((steps * (steps - 1) // 2, rank, sides))],
        scratch_shapes=[pltpu.VMEM((n_row, rows, keep), BF)],
        cost_estimate=cost(10**8, 10**6),
        name="settle",
    )(idx, *messages)


def answer_of(idx, answers, final, steps, sides, rank):
    n_row = len(answers)
    width, ts = answers[0].shape

    def kernel(idx_ref, final_ref, *refs):
        r = idx_ref[0]
        held = refs[n_row + 1]
        for d in range(n_row):
            held[r ^ d] = refs[d][...]
        where, n = {}, 0
        for m in range(steps):
            for k in range(m + 1, steps):
                where[k, m] = n
                n += 1
        for m in range(steps):
            out = held[m, :sides].astype(F32).T
            for l in range(m):
                at = sides + l * rank
                out = out - tn(held[m, at : at + rank], final_ref[where[m, l]])
            refs[n_row][m] = out.astype(BF)

    return pl.pallas_call(
        kernel,
        in_specs=[SMEM, VMEM] + [VMEM] * n_row,
        out_specs=VMEM,
        out_shape=sds((steps, ts, sides)),
        scratch_shapes=[pltpu.VMEM((n_row, width, ts), BF)],
        cost_estimate=cost(10**8, 10**6),
        name="answer_of",
    )(idx, final, *answers)


def collect(idx, pieces, masks, slots):
    count = len(pieces)

    def kernel(idx_ref, *refs):
        for n, e in enumerate(masks):
            refs[count][idx_ref[1] ^ e] = refs[n][...]

    return pl.pallas_call(
        kernel,
        in_specs=[SMEM] + [VMEM] * count,
        out_specs=VMEM,
        out_shape=sds((slots,) + pieces[0].shape),
        cost_estimate=cost(10**6, count * pieces[0].size * 4),
        name="collect",
    )(idx, *pieces)


def scatter_sum(blocks, axis, size, low):
    kept = [blocks[at].astype(F32) for at in range(0, size, low)]
    for m in range(1, low):
        sent = jnp.stack([blocks[at + m] for at in range(0, size, low)], 0)
        got = swap(sent, axis, size, m)
        kept = [k + got[n].astype(F32) for n, k in enumerate(kept)]
    total = kept[0]
    for n in range(1, size // low):
        total = total + swap(kept[n].astype(BF), axis, size, n * low).astype(F32)
    return total


def cut(value, index, width, dim):
    return lax.dynamic_slice_in_dim(value, index * width, width, dim)


def plain(n_row, n_col, right_sides, prior_left, prior_right, solved_prior, diag_left, diag_right, diag_inverse):
    ts, slots, sides = right_sides.shape
    rank, tile = prior_left.shape[2:]
    steps = diag_left.shape[1]
    r = lax.axis_index("row")
    c = lax.axis_index("col")
    own = jnp.minimum(r, steps - 1)
    low_c, low_r = low_of(n_col), 2
    chunk = slots * rank // n_col

    known = jnp.concatenate(gather(solved_prior, "row", n_row, low_r), 1)
    tb = tile // n_row
    pr = jnp.concatenate([cut(prior_right, r ^ d, tb, 3) for d in range(n_row)], 3)

    turned = [pick(diag_right, jnp.minimum(r ^ d, steps - 1), 1) for d in range(n_row)]
    factors = [turned[0]] + [swap(turned[d], "row", n_row, d) for d in range(1, n_row)]
    factors = jnp.stack(factors, 0)
    flat = factors.reshape(n_row, n_col, chunk, ts)
    right = [pick(flat, c ^ e, 1).reshape(n_row * chunk, ts) for e in range(n_col)]
    right = [right[0]] + [swap(right[e], "col", n_col, e) for e in range(1, n_col)]
    right = jnp.concatenate(right, 1)
    heads = factors[:, 0].reshape(n_row * rank, ts)
    heads = jnp.concatenate(gather(heads, "col", n_col, low_c), 1)

    inverse = pick(diag_inverse, own)
    inverse = jnp.concatenate([cut(inverse, c ^ e, ts, 1) for e in range(n_col)], 1)

    lead_left = [cut(prior_left[0], c ^ e, ts, 2) for e in range(n_col)]

    coeff = jnp.einsum("jth,jrt->jrh", known, pr[0], preferred_element_type=F32).astype(BF)
    parts = [
        jnp.einsum("jrh,jrt->ht", coeff, lead_left[e], preferred_element_type=F32).astype(BF)
        for e in range(n_col)
    ]
    lead = right_sides[:, 0].astype(F32).T - scatter_sum(parts, "col", n_col, low_c)
    lefts = diag_left[0, : steps - 1].reshape((steps - 1) * rank, ts)
    wide = jnp.concatenate([lead.astype(BF), lefts], 0)
    wide = jnp.concatenate(gather(wide, "col", n_col, low_c), 1)
    answer = jnp.einsum("ws,ts->wt", wide, inverse, preferred_element_type=F32).astype(BF)
    answers = gather(answer, "row", n_row, low_r)
    full = jnp.concatenate(gather(answer, "col", n_col, low_c), 1)
    near = jnp.einsum("qt,wt->qw", right, full, preferred_element_type=F32).astype(BF)
    near = near.reshape(n_row, chunk, -1)
    head = jnp.einsum("qt,wt->qw", heads, full, preferred_element_type=F32).astype(BF)
    head = head.reshape(n_row, rank, -1)
    near = jnp.stack([near[0]] + [swap(near[d], "row", n_row, d) for d in range(1, n_row)], 0)
    head = gather(head, "row", n_row, low_r)
    head = jnp.stack(head, 0)
    near = [pick(near, r ^ m).astype(F32) for m in range(steps)]
    heads_of = {}
    for m in range(steps):
        mine = pick(head, r ^ m)
        for k in range(m + 1, steps):
            heads_of[k, m] = mine[k ^ m].astype(F32)

    def fixed(value, m, known_c):
        out = value[:, :sides]
        for l in range(m):
            at = sides + l * rank
            out = out - jnp.dot(value[:, at : at + rank].astype(BF), known_c[m, l], preferred_element_type=F32)
        return out.astype(BF)

    known_c = {}
    for m in range(steps):
        for k in range(m + 1, steps):
            known_c[k, m] = fixed(heads_of[k, m], m, known_c)
    slot_of = (c * chunk + jnp.arange(chunk)) // rank
    mine = jnp.stack(
        [
            jnp.where((slot_of * n_row + r > m)[:, None], fixed(near[m], m, known_c), 0).astype(BF)
            for m in range(steps)
        ],
        0,
    )
    pieces = jnp.stack(gather(mine, "col", n_col, low_c), 0)
    pieces = jnp.stack([pick(pieces, c ^ n) for n in range(n_col)], 0)
    every = jnp.moveaxis(pieces, 0, 1).reshape(steps, slots, rank, sides)

    answers = jnp.stack(answers, 0)
    solved = []
    for m in range(steps):
        a = pick(answers, r ^ m).astype(F32)
        out = a[:sides].T
        for l in range(m):
            at = sides + l * rank
            out = out - jnp.einsum("rt,rh->th", a[at : at + rank].astype(BF), known_c[m, l], preferred_element_type=F32)
        solved.append(out.astype(BF))
    solved = jnp.stack(solved, 0)

    rest = jnp.einsum("jth,sjrt->sjrh", known, pr[1:], preferred_element_type=F32).astype(BF)
    rest = jnp.einsum("sjrt,sjrh->tsh", prior_left[1:], rest, preferred_element_type=F32).astype(BF)
    rest = lax.psum_scatter(rest, "col", scatter_dimension=0, tiled=True).astype(F32)
    base = jnp.concatenate([lead.T[:, None], right_sides[:, 1:].astype(F32) - rest], 1)
    updated = base - jnp.einsum("smrt,msrh->tsh", diag_left, every, preferred_element_type=F32)
    return updated, solved


def local(n_row, n_col, *args):
    right_sides, _, _, _, diag_left, _, _ = args
    ts, slots, _ = right_sides.shape
    steps = diag_left.shape[1]
    if ts % 128 or n_row != steps or n_col != slots:
        return plain(n_row, n_col, *args)
    return tiled(n_row, n_col, *args)


def tiled(n_row, n_col, right_sides, prior_left, prior_right, solved_prior, diag_left, diag_right, diag_inverse):
    ts, slots, sides = right_sides.shape
    rank = prior_left.shape[2]
    steps = diag_left.shape[1]
    r = lax.axis_index("row")
    c = lax.axis_index("col")
    idx = jnp.stack([r, c, r]).astype(jnp.int32)
    low = low_of(n_col)
    nz = n_col // low
    half = slots // 2
    groups = (1, half, slots - 1 - half)

    def send(value, axis, mask):
        return swap(value, axis, n_row if axis == "row" else n_col, mask)

    def spread(value, axis, direct=False):
        size = n_row if axis == "row" else n_col
        result = [value] + [None] * (size - 1)
        if direct:
            for at in range(low, size, low):
                result[at] = send(value, axis, at)
            for at in range(0, size, low):
                for m in range(1, low):
                    result[at + m] = send(result[at], axis, m)
            return result
        mask = size // 2
        while mask:
            for at in range(0, size, 2 * mask):
                result[at + mask] = send(result[at], axis, mask)
            mask //= 2
        return result

    known = spread(solved_prior, "row")
    factors, side = pack_right(diag_right, right_sides)
    factors = lax.all_to_all(factors, "col", 0, 0)
    packed = pack_left(idx, prior_left, low, nz, ts)
    packed = [packed[0]] + [send(packed[m], "col", m) for m in range(1, low)]
    coeffs = coefficients(idx, known, prior_right, groups)
    leads = [coeffs[0]] + [send(coeffs[0], "col", m) for m in range(1, low)]
    factors = lax.all_to_all(jnp.transpose(factors, (1, 0, 2, 3)), "row", 0, 0)

    parts = lead_parts(leads, packed, nz, ts)
    parts = [parts[0]] + [send(parts[k], "col", k * low) for k in range(1, nz)]
    wide, lead = widen(parts, side, diag_left, steps - 1)
    wide = spread(wide, "col")
    answer = solve(idx, wide, diag_inverse)
    full = spread(answer, "col")
    answers = spread(answer, "row")
    messages = nears(idx, full, factors, rank, rank)
    messages = [messages[0]] + [send(messages[d], "row", d) for d in range(1, n_row)]
    mine, final = settle(idx, messages, steps, sides, rank, rank, 1)
    pieces = spread(mine, "col", True)
    solved = answer_of(idx, answers, final, steps, sides, rank)

    order = [0]
    while len(order) < nz:
        order = [2 * k for k in order] + [2 * k + 1 for k in order]
    blocks = [[m + k * low for k in order] for m in range(low)]
    rest = []
    for n in range(1, len(groups)):
        parts = rest_parts(idx, coeffs[n], prior_left, sum(groups[:n]), blocks, ts)
        gots = [send(parts[m], "col", m) for m in range(1, low)]
        kept, mask = parts[0], low
        while True:
            half = kept.shape[0] // 2
            if half == 0:
                break

            def added(part):
                total = kept[part].astype(F32)
                for got in gots:
                    total = total + got[part].astype(F32)
                return total.astype(BF)

            sent = added(slice(half, None))
            kept = added(slice(0, half))
            gots, mask = [send(sent, "col", mask)], 2 * mask
        rest.append(kept[0].astype(F32) + gots[0][0].astype(F32))
    rest = jnp.concatenate(rest, 0)
    late = tuple(at + m for at in range(low, n_col, low) for m in range(1, low))
    early = tuple(e for e in range(n_col) if e not in late)
    every = collect(idx, [pieces[e] for e in early], early, slots)
    for e in late:
        every = lax.dynamic_update_index_in_dim(every, pieces[e], c ^ e, 0)
    base = jnp.concatenate([lead.T[:, None], right_sides[:, 1:].astype(F32) - jnp.transpose(rest, (2, 0, 1))], 1)
    updated = base - jnp.einsum("smrt,smrh->tsh", diag_left, every, preferred_element_type=F32)
    return updated, solved


def solution(mesh):
    n_row, n_col = mesh.shape["row"], mesh.shape["col"]
    in_specs = (
        P("col", "row", None),
        P("row", "col", None, None),
        P("row", "col", None, None),
        P("col", "row", None),
        P("row", None, None, "col"),
        P("row", None, None, "col"),
        P(None, "col", None),
    )
    out_specs = (P("col", "row", None), P(None, "col", None))

    def body(*args):
        return local(n_row, n_col, *args)

    return jax.shard_map(body, mesh=mesh, in_specs=in_specs, out_specs=out_specs, check_vma=False)
```

```python
import jax
import jax.numpy as jnp
from jax import lax
from jax.experimental import pallas as pl
from jax.experimental.pallas import tpu as pltpu
from jax.sharding import PartitionSpec as P


BF = jnp.bfloat16
F32 = jnp.float32
SMEM = pl.BlockSpec(memory_space=pltpu.SMEM)
VMEM = pl.BlockSpec(memory_space=pltpu.VMEM)


def swap(value, axis, size, mask):
    return lax.ppermute(value, axis, [(i, i ^ mask) for i in range(size)])


def low_of(size):
    return 2 if size <= 8 else 4


def gather(value, axis, size, low):
    own = [value] + [swap(value, axis, size, m) for m in range(low, size, low)]
    result = [None] * size
    for at, piece in enumerate(own):
        result[at * low] = piece
        for m in range(1, low):
            result[at * low + m] = swap(piece, axis, size, m)
    return result


def pick(value, index, dim=0):
    return lax.dynamic_index_in_dim(value, index, dim, keepdims=False)


def tn(a, b):
    return lax.dot_general(a, b, (((0,), (0,)), ((), ())), preferred_element_type=F32)


def nt(a, b):
    return lax.dot_general(a, b, (((1,), (1,)), ((), ())), preferred_element_type=F32)


def nn(a, b):
    return lax.dot_general(a, b, (((1,), (0,)), ((), ())), preferred_element_type=F32)


def sds(shape, dtype=BF):
    return jax.ShapeDtypeStruct(shape, dtype)


def cost(flops, size):
    return pl.CostEstimate(flops=flops, bytes_accessed=size, transcendentals=0)


def pack_left(idx, left, low, nz, ts):
    _, js, rank, tile = left.shape

    def kernel(idx_ref, in_ref, *outs):
        c = idx_ref[1]
        for m in range(low):
            for k in range(nz):
                at = pl.multiple_of((c ^ (m + k * low)) * ts, ts)
                outs[m][:, k * ts : (k + 1) * ts] = in_ref[0, :, :, pl.ds(at, ts)].reshape(js * rank, ts)

    return pl.pallas_call(
        kernel,
        grid=(1,),
        in_specs=[SMEM, pl.BlockSpec((1, js, rank, tile), lambda n: (0, 0, 0, 0))],
        out_specs=[pl.BlockSpec((js * rank, nz * ts), lambda n: (0, 0))] * low,
        out_shape=[sds((js * rank, nz * ts))] * low,
        cost_estimate=cost(10**6, js * rank * tile * 4),
        name="pack_left",
    )(idx, left)


def pack_right(right, side):
    slots, steps, rank, ts = right.shape
    sides = side.shape[2]

    def kernel(in_ref, side_ref, out_ref, first_ref):
        out_ref[:, :, :rank] = in_ref[...]
        for s in range(slots):
            out_ref[s, :, rank:] = in_ref[0]
        first_ref[...] = side_ref[:, 0, :].astype(F32).T

    return pl.pallas_call(
        kernel,
        in_specs=[VMEM] * 2,
        out_specs=[VMEM] * 2,
        out_shape=[sds((slots, steps, 2 * rank, ts)), sds((sides, ts), F32)],
        cost_estimate=cost(10**6, right.size * 6),
        name="pack_right",
    )(right, side)


def coefficients(idx, known, right, groups):
    n_row = len(known)
    slots, js, rank, tile = right.shape
    tb, sides = known[0].shape[1:]

    def kernel(idx_ref, right_ref, *refs):
        r = idx_ref[0]
        held = refs[-1]
        for d in range(n_row):
            held[:, pl.ds(pl.multiple_of((r ^ d) * tb, tb), tb)] = refs[d][...]
        for j in range(js):
            total = nn(right_ref[:, j].reshape(slots * rank, tile), held[j])
            total = total.astype(BF).reshape(slots, rank, sides)
            at = 0
            for n, count in enumerate(groups):
                refs[n_row + n][:, j * rank : (j + 1) * rank] = total[at : at + count]
                at += count

    return pl.pallas_call(
        kernel,
        in_specs=[SMEM] + [VMEM] * (n_row + 1),
        out_specs=[VMEM] * len(groups),
        out_shape=[sds((g, js * rank, sides)) for g in groups],
        scratch_shapes=[pltpu.VMEM((js, tile, sides), BF)],
        cost_estimate=cost(2 * slots * js * rank * tile * sides, right.size * 2 + n_row * known[0].size * 2),
        name="coefficients",
    )(idx, right, *known)


def lead_parts(coeffs, lefts, nz, ts):
    low = len(coeffs)
    sides = coeffs[0].shape[2]

    def kernel(*refs):
        total = tn(refs[0][0], refs[low][...])
        for m in range(1, low):
            total = total + tn(refs[m][0], refs[low + m][...])
        for k in range(nz):
            refs[2 * low + k][...] = total[:, k * ts : (k + 1) * ts].astype(BF)

    return pl.pallas_call(
        kernel,
        in_specs=[VMEM] * (2 * low),
        out_specs=[VMEM] * nz,
        out_shape=[sds((sides, ts))] * nz,
        cost_estimate=cost(2 * low * lefts[0].size * sides, 10**6),
        name="lead_parts",
    )(*coeffs, *lefts)


def rest_parts(idx, coeff, left, first, blocks, ts):
    count, ranks, sides = coeff.shape
    _, js, rank, tile = left.shape
    many = len(blocks[0])

    def kernel(idx_ref, coeff_ref, left_ref, *refs):
        c = idx_ref[1]
        held = refs[-1]
        flat = [e for block in blocks for e in block]
        for n, e in enumerate(flat):
            at = pl.multiple_of((c ^ e) * ts, ts)
            held[:, n * ts : (n + 1) * ts] = left_ref[0, :, :, pl.ds(at, ts)].reshape(ranks, ts)
        total = tn(coeff_ref[0], held[...])
        for n in range(len(flat)):
            refs[n // many][n % many, 0] = total[:, n * ts : (n + 1) * ts].astype(BF)

    return pl.pallas_call(
        kernel,
        grid=(count,),
        in_specs=[
            SMEM,
            pl.BlockSpec((1, ranks, sides), lambda s: (s, 0, 0)),
            pl.BlockSpec((1, js, rank, tile), lambda s: (s + first, 0, 0, 0)),
        ],
        out_specs=[pl.BlockSpec((many, 1, sides, ts), lambda s: (0, s, 0, 0))] * len(blocks),
        out_shape=[sds((many, count, sides, ts))] * len(blocks),
        scratch_shapes=[pltpu.VMEM((ranks, tile), BF)],
        cost_estimate=cost(2 * count * ranks * sides * tile, count * (ranks * (sides + tile) + tile * sides) * 2),
        name="rest_parts",
    )(idx, coeff, left)


def widen(parts, side, left, extra):
    count = len(parts)
    sides, ts = parts[0].shape
    rank = left.shape[2]

    def kernel(*refs):
        total = refs[0][...].astype(F32)
        for n in range(1, count):
            total = total + refs[n][...].astype(F32)
        lead = refs[count][...] - total
        refs[count + 2][:sides] = lead.astype(BF)
        refs[count + 2][sides:] = refs[count + 1][0, :extra].reshape(extra * rank, ts)
        refs[count + 3][...] = lead

    return pl.pallas_call(
        kernel,
        grid=(1,),
        in_specs=[pl.BlockSpec((sides, ts), lambda n: (0, 0))] * (count + 1)
        + [pl.BlockSpec((1,) + left.shape[1:], lambda n: (0, 0, 0, 0))],
        out_specs=[pl.BlockSpec((sides + extra * rank, ts), lambda n: (0, 0)), pl.BlockSpec((sides, ts), lambda n: (0, 0))],
        out_shape=[sds((sides + extra * rank, ts)), sds((sides, ts), F32)],
        cost_estimate=cost(10**6, 10**6),
        name="widen",
    )(*parts, side, left)


def solve(idx, pieces, inverse):
    n_col = len(pieces)
    width, ts = pieces[0].shape
    _, _, tile = inverse.shape

    def kernel(idx_ref, inverse_ref, *refs):
        c = idx_ref[1]
        held = refs[-1]
        for e in range(n_col):
            held[:, pl.ds(pl.multiple_of((c ^ e) * ts, ts), ts)] = refs[e][...]
        refs[n_col][...] = nt(held[...], inverse_ref[0]).astype(BF)

    return pl.pallas_call(
        kernel,
        grid_spec=pltpu.PrefetchScalarGridSpec(
            num_scalar_prefetch=1,
            grid=(1,),
            in_specs=[pl.BlockSpec((1, ts, tile), lambda n, ref: (ref[2], 0, 0))]
            + [pl.BlockSpec((width, ts), lambda n, ref: (0, 0))] * n_col,
            out_specs=pl.BlockSpec((width, ts), lambda n, ref: (0, 0)),
            scratch_shapes=[pltpu.VMEM((width, tile), BF)],
        ),
        out_shape=sds((width, ts)),
        cost_estimate=cost(2 * width * ts * tile, 2 * ts * tile + 2 * width * tile),
        name="solve",
    )(idx, inverse, *pieces)


def folded(width, rank, q):
    keep = width // 128 * 128
    return keep if q <= rank and width - rank + (width - keep) <= keep else width


def nears(idx, pieces, right, q, rank):
    n_col = len(pieces)
    n_row, _, both_ranks, _ = right.shape
    width, ts = pieces[0].shape
    tile = n_col * ts
    rows = q + (n_row - 1) * rank
    keep = folded(width, rank, q)

    def kernel(idx_ref, right_ref, *refs):
        r, c = idx_ref[0], idx_ref[1]
        out, held, factor, both = refs[n_col : n_col + n_row], refs[-3], refs[-2], refs[-1]
        for e in range(n_col):
            held[:, pl.ds(pl.multiple_of((c ^ e) * ts, ts), ts)] = refs[e][...]
            factor[:, :, e * ts : (e + 1) * ts] = right_ref[:, e]
        product = nt(factor[...].reshape(n_row * both_ranks, tile), held[...])
        both[...] = product.astype(BF).reshape(n_row, both_ranks, width)
        for d in range(n_row):
            out[d][:q] = both[r ^ d, :q, :keep]
            for k in range(1, n_row):
                out[d][q + (k - 1) * rank : q + k * rank] = both[k, q:, :keep]
            if keep < width:
                out[d][q : 2 * q, width - rank : width - rank + width - keep] = both[r ^ d, :q, keep:]

    return pl.pallas_call(
        kernel,
        in_specs=[SMEM] + [VMEM] * (n_col + 1),
        out_specs=[VMEM] * n_row,
        out_shape=[sds((rows, keep))] * n_row,
        scratch_shapes=[
            pltpu.VMEM((width, tile), BF),
            pltpu.VMEM((n_row, both_ranks, tile), BF),
            pltpu.VMEM((n_row, both_ranks, width), BF),
        ],
        cost_estimate=cost(2 * n_row * both_ranks * width * tile, 10**6),
        name="nears",
    )(idx, right, *pieces)


def settle(idx, messages, steps, sides, q, rank, per):
    n_row = len(messages)
    rows, keep = messages[0].shape
    width = sides + (steps - 1) * rank

    def kernel(idx_ref, *refs):
        r, c = idx_ref[0], idx_ref[1]
        held = refs[n_row + 2]
        for d in range(n_row):
            held[r ^ d] = refs[d][...]
        final = {}

        def fixed(value, m):
            out = value[:, :sides].astype(F32)
            for l in range(m):
                at = sides + l * rank
                out = out - nn(value[:, at : at + rank], final[m, l])
            return out.astype(BF)

        at_final = 0
        for m in range(steps):
            for k in range(m + 1, steps):
                at = q + (k - 1) * rank
                final[k, m] = fixed(held[m, at : at + rank], m)
                refs[n_row + 1][at_final] = final[k, m]
                at_final += 1
        slot = c // per
        for m in range(steps):
            mine = held[m, :q]
            if keep < width and m == steps - 1:
                mine = jnp.concatenate([mine, held[m, q : 2 * q, width - rank : width - rank + width - keep]], 1)
            mine = fixed(mine, m)
            refs[n_row][m] = jnp.where(slot * n_row + r > m, mine, jnp.zeros_like(mine))

    return pl.pallas_call(
        kernel,
        in_specs=[SMEM] + [VMEM] * n_row,
        out_specs=[VMEM] * 2,
        out_shape=[sds((steps, q, sides)), sds((steps * (steps - 1) // 2, rank, sides))],
        scratch_shapes=[pltpu.VMEM((n_row, rows, keep), BF)],
        cost_estimate=cost(10**8, 10**6),
        name="settle",
    )(idx, *messages)


def answer_of(idx, answers, final, steps, sides, rank):
    n_row = len(answers)
    width, ts = answers[0].shape

    def kernel(idx_ref, final_ref, *refs):
        r = idx_ref[0]
        held = refs[n_row + 1]
        for d in range(n_row):
            held[r ^ d] = refs[d][...]
        where, n = {}, 0
        for m in range(steps):
            for k in range(m + 1, steps):
                where[k, m] = n
                n += 1
        for m in range(steps):
            out = held[m, :sides].astype(F32).T
            for l in range(m):
                at = sides + l * rank
                out = out - tn(held[m, at : at + rank], final_ref[where[m, l]])
            refs[n_row][m] = out.astype(BF)

    return pl.pallas_call(
        kernel,
        in_specs=[SMEM, VMEM] + [VMEM] * n_row,
        out_specs=VMEM,
        out_shape=sds((steps, ts, sides)),
        scratch_shapes=[pltpu.VMEM((n_row, width, ts), BF)],
        cost_estimate=cost(10**8, 10**6),
        name="answer_of",
    )(idx, final, *answers)


def collect(idx, pieces, masks, slots):
    count = len(pieces)

    def kernel(idx_ref, *refs):
        for n, e in enumerate(masks):
            refs[count][idx_ref[1] ^ e] = refs[n][...]

    return pl.pallas_call(
        kernel,
        in_specs=[SMEM] + [VMEM] * count,
        out_specs=VMEM,
        out_shape=sds((slots,) + pieces[0].shape),
        cost_estimate=cost(10**6, count * pieces[0].size * 4),
        name="collect",
    )(idx, *pieces)


def scatter_sum(blocks, axis, size, low):
    kept = [blocks[at].astype(F32) for at in range(0, size, low)]
    for m in range(1, low):
        sent = jnp.stack([blocks[at + m] for at in range(0, size, low)], 0)
        got = swap(sent, axis, size, m)
        kept = [k + got[n].astype(F32) for n, k in enumerate(kept)]
    total = kept[0]
    for n in range(1, size // low):
        total = total + swap(kept[n].astype(BF), axis, size, n * low).astype(F32)
    return total


def cut(value, index, width, dim):
    return lax.dynamic_slice_in_dim(value, index * width, width, dim)


def plain(n_row, n_col, right_sides, prior_left, prior_right, solved_prior, diag_left, diag_right, diag_inverse):
    ts, slots, sides = right_sides.shape
    rank, tile = prior_left.shape[2:]
    steps = diag_left.shape[1]
    r = lax.axis_index("row")
    c = lax.axis_index("col")
    own = jnp.minimum(r, steps - 1)
    low_c, low_r = low_of(n_col), 2
    chunk = slots * rank // n_col

    known = jnp.concatenate(gather(solved_prior, "row", n_row, low_r), 1)
    tb = tile // n_row
    pr = jnp.concatenate([cut(prior_right, r ^ d, tb, 3) for d in range(n_row)], 3)

    turned = [pick(diag_right, jnp.minimum(r ^ d, steps - 1), 1) for d in range(n_row)]
    factors = [turned[0]] + [swap(turned[d], "row", n_row, d) for d in range(1, n_row)]
    factors = jnp.stack(factors, 0)
    flat = factors.reshape(n_row, n_col, chunk, ts)
    right = [pick(flat, c ^ e, 1).reshape(n_row * chunk, ts) for e in range(n_col)]
    right = [right[0]] + [swap(right[e], "col", n_col, e) for e in range(1, n_col)]
    right = jnp.concatenate(right, 1)
    heads = factors[:, 0].reshape(n_row * rank, ts)
    heads = jnp.concatenate(gather(heads, "col", n_col, low_c), 1)

    inverse = pick(diag_inverse, own)
    inverse = jnp.concatenate([cut(inverse, c ^ e, ts, 1) for e in range(n_col)], 1)

    lead_left = [cut(prior_left[0], c ^ e, ts, 2) for e in range(n_col)]

    coeff = jnp.einsum("jth,jrt->jrh", known, pr[0], preferred_element_type=F32).astype(BF)
    parts = [
        jnp.einsum("jrh,jrt->ht", coeff, lead_left[e], preferred_element_type=F32).astype(BF)
        for e in range(n_col)
    ]
    lead = right_sides[:, 0].astype(F32).T - scatter_sum(parts, "col", n_col, low_c)
    lefts = diag_left[0, : steps - 1].reshape((steps - 1) * rank, ts)
    wide = jnp.concatenate([lead.astype(BF), lefts], 0)
    wide = jnp.concatenate(gather(wide, "col", n_col, low_c), 1)
    answer = jnp.einsum("ws,ts->wt", wide, inverse, preferred_element_type=F32).astype(BF)
    answers = gather(answer, "row", n_row, low_r)
    full = jnp.concatenate(gather(answer, "col", n_col, low_c), 1)
    near = jnp.einsum("qt,wt->qw", right, full, preferred_element_type=F32).astype(BF)
    near = near.reshape(n_row, chunk, -1)
    head = jnp.einsum("qt,wt->qw", heads, full, preferred_element_type=F32).astype(BF)
    head = head.reshape(n_row, rank, -1)
    near = jnp.stack([near[0]] + [swap(near[d], "row", n_row, d) for d in range(1, n_row)], 0)
    head = gather(head, "row", n_row, low_r)
    head = jnp.stack(head, 0)
    near = [pick(near, r ^ m).astype(F32) for m in range(steps)]
    heads_of = {}
    for m in range(steps):
        mine = pick(head, r ^ m)
        for k in range(m + 1, steps):
            heads_of[k, m] = mine[k ^ m].astype(F32)

    def fixed(value, m, known_c):
        out = value[:, :sides]
        for l in range(m):
            at = sides + l * rank
            out = out - jnp.dot(value[:, at : at + rank].astype(BF), known_c[m, l], preferred_element_type=F32)
        return out.astype(BF)

    known_c = {}
    for m in range(steps):
        for k in range(m + 1, steps):
            known_c[k, m] = fixed(heads_of[k, m], m, known_c)
    slot_of = (c * chunk + jnp.arange(chunk)) // rank
    mine = jnp.stack(
        [
            jnp.where((slot_of * n_row + r > m)[:, None], fixed(near[m], m, known_c), 0).astype(BF)
            for m in range(steps)
        ],
        0,
    )
    pieces = jnp.stack(gather(mine, "col", n_col, low_c), 0)
    pieces = jnp.stack([pick(pieces, c ^ n) for n in range(n_col)], 0)
    every = jnp.moveaxis(pieces, 0, 1).reshape(steps, slots, rank, sides)

    answers = jnp.stack(answers, 0)
    solved = []
    for m in range(steps):
        a = pick(answers, r ^ m).astype(F32)
        out = a[:sides].T
        for l in range(m):
            at = sides + l * rank
            out = out - jnp.einsum("rt,rh->th", a[at : at + rank].astype(BF), known_c[m, l], preferred_element_type=F32)
        solved.append(out.astype(BF))
    solved = jnp.stack(solved, 0)

    rest = jnp.einsum("jth,sjrt->sjrh", known, pr[1:], preferred_element_type=F32).astype(BF)
    rest = jnp.einsum("sjrt,sjrh->tsh", prior_left[1:], rest, preferred_element_type=F32).astype(BF)
    rest = lax.psum_scatter(rest, "col", scatter_dimension=0, tiled=True).astype(F32)
    base = jnp.concatenate([lead.T[:, None], right_sides[:, 1:].astype(F32) - rest], 1)
    updated = base - jnp.einsum("smrt,msrh->tsh", diag_left, every, preferred_element_type=F32)
    return updated, solved


def local(n_row, n_col, *args):
    right_sides, _, _, _, diag_left, _, _ = args
    ts, slots, _ = right_sides.shape
    steps = diag_left.shape[1]
    if ts % 128 or n_row != steps or n_col != slots:
        return plain(n_row, n_col, *args)
    return tiled(n_row, n_col, *args)


def tiled(n_row, n_col, right_sides, prior_left, prior_right, solved_prior, diag_left, diag_right, diag_inverse):
    ts, slots, sides = right_sides.shape
    rank = prior_left.shape[2]
    steps = diag_left.shape[1]
    r = lax.axis_index("row")
    c = lax.axis_index("col")
    idx = jnp.stack([r, c, r]).astype(jnp.int32)
    low = low_of(n_col)
    nz = n_col // low
    half = slots // 2
    groups = (1, half, slots - 1 - half)

    def send(value, axis, mask):
        return swap(value, axis, n_row if axis == "row" else n_col, mask)

    def spread(value, axis, direct=False):
        size = n_row if axis == "row" else n_col
        result = [value] + [None] * (size - 1)
        if direct:
            for at in range(low, size, low):
                result[at] = send(value, axis, at)
            for at in range(0, size, low):
                for m in range(1, low):
                    result[at + m] = send(result[at], axis, m)
            return result
        mask = size // 2
        while mask:
            for at in range(0, size, 2 * mask):
                result[at + mask] = send(result[at], axis, mask)
            mask //= 2
        return result

    known = spread(solved_prior, "row")
    factors, side = pack_right(diag_right, right_sides)
    factors = lax.all_to_all(factors, "col", 0, 0)
    packed = pack_left(idx, prior_left, low, nz, ts)
    packed = [packed[0]] + [send(packed[m], "col", m) for m in range(1, low)]
    coeffs = coefficients(idx, known, prior_right, groups)
    leads = [coeffs[0]] + [send(coeffs[0], "col", m) for m in range(1, low)]
    factors = lax.all_to_all(jnp.transpose(factors, (1, 0, 2, 3)), "row", 0, 0)

    parts = lead_parts(leads, packed, nz, ts)
    parts = [parts[0]] + [send(parts[k], "col", k * low) for k in range(1, nz)]
    wide, lead = widen(parts, side, diag_left, steps - 1)
    wide = spread(wide, "col")
    answer = solve(idx, wide, diag_inverse)
    full = spread(answer, "col")
    answers = spread(answer, "row")
    messages = nears(idx, full, factors, rank, rank)
    messages = [messages[0]] + [send(messages[d], "row", d) for d in range(1, n_row)]
    mine, final = settle(idx, messages, steps, sides, rank, rank, 1)
    pieces = spread(mine, "col", True)
    solved = answer_of(idx, answers, final, steps, sides, rank)

    order = [0]
    while len(order) < nz:
        order = [2 * k for k in order] + [2 * k + 1 for k in order]
    blocks = [[m + k * low for k in order] for m in range(low)]
    rest = []
    for n in range(1, len(groups)):
        parts = rest_parts(idx, coeffs[n], prior_left, sum(groups[:n]), blocks, ts)
        gots = [send(parts[m], "col", m) for m in range(1, low)]
        kept, mask = parts[0], low
        while True:
            half = kept.shape[0] // 2
            if half == 0:
                break

            def added(part):
                total = kept[part].astype(F32)
                for got in gots:
                    total = total + got[part].astype(F32)
                return total.astype(BF)

            sent = added(slice(half, None))
            kept = added(slice(0, half))
            gots, mask = [send(sent, "col", mask)], 2 * mask
        rest.append(kept[0].astype(F32) + gots[0][0].astype(F32))
    rest = jnp.concatenate(rest, 0)
    late = tuple(at + m for at in range(low, n_col, low) for m in range(1, low))
    early = tuple(e for e in range(n_col) if e not in late)
    every = collect(idx, [pieces[e] for e in early], early, slots)
    for e in late:
        every = lax.dynamic_update_index_in_dim(every, pieces[e], c ^ e, 0)
    base = jnp.concatenate([lead.T[:, None], right_sides[:, 1:].astype(F32) - jnp.transpose(rest, (2, 0, 1))], 1)
    updated = base - jnp.einsum("smrt,smrh->tsh", diag_left, every, preferred_element_type=F32)
    return updated, solved


def solution(mesh):
    n_row, n_col = mesh.shape["row"], mesh.shape["col"]
    in_specs = (
        P("col", "row", None),
        P("row", "col", None, None),
        P("row", "col", None, None),
        P("col", "row", None),
        P("row", None, None, "col"),
        P("row", None, None, "col"),
        P(None, "col", None),
    )
    out_specs = (P("col", "row", None), P(None, "col", None))

    def body(*args):
        return local(n_row, n_col, *args)

    return jax.shard_map(body, mesh=mesh, in_specs=in_specs, out_specs=out_specs, check_vma=False)
```
